32 devices in a mesh: groups: 2 (over x), ep: 8 (over z, y), node: 2 (over core).
Axes of the slice: x: 2, y: 2, z: 4, core: 2. Of those that a mesh axis runs over, the one named last changes fastest.
Arguments:
- tokens: bfloat16 [1024, 7168], P(('groups', 'ep', 'node')), parts along dimension 0, may hold values from -6 to 6
- expert_ids: int32 [1024, 8], P(('groups', 'ep', 'node')), parts along dimension 0, may hold values from 0 to 15, all different within a row; in each aligned block of 32 rows (0 to 31, 32 to 63, ...) at most 32 rows name the same one
- gate_weights: float32 [1024, 8], P(('groups', 'ep', 'node')), parts along dimension 0, may hold values from 0.05 to 0.5
- gate_up_weight: bfloat16 [16, 7168, 512], P(('ep', 'node')), may hold values from -0.0625 to 0.0625
- down_weight: bfloat16 [16, 256, 7168], P(('ep', 'node')), may hold values from -0.375 to 0.375
Outputs:
- moe_out: bfloat16 [1024, 7168], P(('groups', 'ep', 'node')), parts along dimension 0
The draws below stay inside these ranges and needn't reach their ends.
There are 2 independent parts, one for each index of `groups`. The reference program is written for one: setup_inputs(seed, part) draws one part's arguments, and reference() takes and returns one part's arrays. A program takes and returns all parts, laid end to end along the dimension named above; an argument that names none is the same for every part. Nothing has to cross between parts.
Inputs may be any that keep to these rules, and one draw needn't show every extreme that they name: `expert_ids`: each token names 8 different experts; among the 32 tokens of one device no expert is named by more than 32 of them, a bound that some block reaches.
All inputs are finite; a program needn't handle non-finite values.
Results may differ from the reference program's by a relative error of at most 0.0058.
Values may be sent and summed in bfloat16 or wider, within the bound.
No kernel may reach another device: no remote copies, remote signals or barrier semaphores. Data moves between devices by JAX's collectives and lax.ppermute only.
A program may use at most 128 MiB of HBM per device.

```python
import math
import jax
import jax.numpy as jnp
import numpy as np
from jax import lax

D = 7168
TOP = 8
EXP_HID = 256
TOK_DEV = 32
EXPERTS = 16
CAP = 32
TOKENS = 512
N_EP = 8
N_NODE = 2


def level_of(rng, dims, split, smallest, high):
    level = 1.0
    for axis_at, blocks in split:
        heights = jax.random.uniform(jax.random.fold_in(jax.random.fold_in(rng, 6), axis_at), (blocks,), jnp.float32, smallest / len(split), high / len(split))
        level = level * jnp.repeat(jnp.exp(heights), dims[axis_at] // blocks).reshape((-1,) + (1,) * (len(dims) - 1 - axis_at))
    return level


def assign_block(rng, own, number, rows, count, top, most, slope):
    sequence = jax.random.permutation(rng, count)
    heavy_load, common = load_shares(count, rows * top, most, slope, True), load_shares(count, rows * top, most, slope, False)
    places = jnp.arange(count)

    def named(sizes, turn):
        used = int((sizes > 0).sum())
        fixed = max(1, used // 4)
        shifted = fixed + (places - fixed + turn * (used - fixed)) % max(1, count - fixed)
        return jnp.zeros((count,), jnp.int32).at[sequence[jnp.where(places < fixed, places, shifted)]].set(jnp.asarray(sizes, jnp.int32))

    sizes = jnp.where(number % 4 == 0, named(heavy_load, number // 4), named(common, number - number // 4 - 1))
    mixed = jax.random.permutation(jax.random.fold_in(own, 3), count)
    source_of, taker = mixed[0:count // 2 * 2:2], mixed[1:count // 2 * 2:2]
    room = jnp.minimum(sizes[source_of] - 1, most - sizes[taker]) // 2
    room = jnp.where((source_of == sequence[0]) | (taker == sequence[0]) | (sizes[taker] == 0), 0, jnp.maximum(room, 0))
    shifted = jax.random.randint(jax.random.fold_in(own, 4), (count // 2,), 0, 1 << 20) % (room + 1)
    sizes = sizes.at[source_of].add(-shifted).at[taker].add(shifted)
    members = jnp.searchsorted(jnp.cumsum(sizes), jnp.arange(rows * top), side="right").astype(jnp.int32)
    table = members.reshape(top, rows).T
    table = table[jax.random.permutation(jax.random.fold_in(own, 1), rows)]
    turn = jax.random.randint(jax.random.fold_in(own, 2), (rows, 1), 0, top)
    return jnp.take_along_axis(table, (jnp.arange(top)[None, :] + turn) % top, axis=1)


def load_shares(amount, total, reach, skew, full):
    weights = [(1 << 20) // math.isqrt(grade ** skew) + 1 for grade in range(1, amount + 1)]
    largest = reach if full else min(reach, max(-(-total // amount), total * weights[0] // sum(weights)))
    least = 1 if total - largest >= amount - 1 else 0
    given, rest = [largest] + [least] * (amount - 1), total - largest - least * (amount - 1)
    while rest > 0:
        free = [i for i in range(1, amount) if given[i] < largest] or [i for i in range(1, amount) if given[i] < reach]
        pool, left = sum([weights[i] for i in free]), rest
        for i in free:
            extra = min(reach - given[i], max(1, left * weights[i] // pool), rest)
            given[i] = given[i] + extra
            rest = rest - extra
    return np.array(given)


def normal_values(key, extent, spread, reach, cuts=(), held_as=jnp.bfloat16):
    drawn = spread * jax.random.normal(key, extent, jnp.float32)
    if cuts:
        drawn = drawn * level_of(key, extent, cuts, -0.22, 0.18)
    return jnp.clip(drawn, -reach, reach).astype(held_as)


def setup_inputs(seed: int = 0, part: int = 0) -> dict:
    splits = jax.random.split(jax.random.key(seed), 6)
    part_keys = jax.random.split(jax.random.fold_in(splits[5], part), 6)
    tokens = normal_values(part_keys[0], (TOKENS, D), 1.0, 6.0, ((0, 16),))
    expert_ids_keys = jax.random.split(jax.random.fold_in(part_keys[1], 1), TOKENS // TOK_DEV)
    expert_ids_turns = jax.random.permutation(jax.random.fold_in(part_keys[1], 3), TOKENS // TOK_DEV)
    expert_ids = jax.vmap(lambda own, number: assign_block(jax.random.fold_in(part_keys[1], 2), own, number, TOK_DEV, EXPERTS, TOP, CAP, 2))(expert_ids_keys, expert_ids_turns).reshape((TOKENS, TOP))
    gate_weights = jnp.clip(jnp.exp(math.log(0.5) - 2.3025851 * jax.random.uniform(part_keys[2], (TOKENS, TOP), jnp.float32) ** level_of(part_keys[2], (TOKENS, TOP), ((0, 16),), -0.2, 0.2)), 0.05, 0.5)
    gate_up_weight = normal_values(splits[3], (EXPERTS, D, 2 * EXP_HID), D ** -0.5, 0.0625, ((0, 16),))
    down_weight = normal_values(splits[4], (EXPERTS, EXP_HID, D), EXP_HID ** -0.5, 0.375, ((0, 16),))
    return {"tokens": tokens, "expert_ids": expert_ids, "gate_weights": gate_weights, "gate_up_weight": gate_up_weight, "down_weight": down_weight}


def reference(tokens, expert_ids, gate_weights, gate_up_weight, down_weight):
    slot_total = N_EP * N_NODE * CAP
    token_index = jnp.arange(TOKENS, dtype=jnp.int32)

    def per_expert(running, expert):
        chosen = expert_ids == expert
        routed = jnp.any(chosen, axis=1)
        picked = jnp.sum(jnp.where(chosen, gate_weights, jnp.zeros_like(gate_weights)), axis=1)
        position = jnp.cumsum(routed.astype(jnp.int32)) - 1
        where_to = jnp.where(routed, position, slot_total).astype(jnp.int32)
        row_index = jnp.zeros((slot_total,), jnp.int32).at[where_to].set(token_index, mode="drop")
        filled = jnp.zeros((slot_total,), jnp.float32).at[where_to].set(jnp.ones((TOKENS,), jnp.float32), mode="drop")
        gathered = tokens[row_index]
        gate_up = jnp.dot(gathered, gate_up_weight[expert], preferred_element_type=jnp.float32)
        hidden = (jax.nn.silu(gate_up[:, :EXP_HID]) * gate_up[:, EXP_HID:]).astype(jnp.bfloat16)
        result = jnp.dot(hidden, down_weight[expert], preferred_element_type=jnp.float32).astype(jnp.bfloat16)
        weight_row = filled * picked[row_index]
        running = running.at[row_index].add(weight_row[:, None] * result.astype(jnp.float32))
        return running, None

    start = jnp.zeros((TOKENS, D), jnp.float32)
    summed, unused = lax.scan(per_expert, start, jnp.arange(EXPERTS, dtype=jnp.int32))
    return summed.astype(jnp.bfloat16)
```

```python
import jax
import jax.numpy as jnp
from jax import lax
from jax.sharding import PartitionSpec as P


CHUNKS = 4


def ring_order(mesh):
    at = mesh.axis_names.index("ep")
    count = mesh.devices.shape[at]
    line = [mesh.devices[tuple(i if d == at else 0 for d in range(mesh.devices.ndim))] for i in range(count)]
    places = [getattr(device, "coords", None) for device in line]
    if any(place is None for place in places):
        return list(range(count))
    varying = [d for d in range(3) if len({place[d] for place in places}) > 1]
    if len(varying) == 2:
        short, long = sorted(varying, key=lambda d: len({place[d] for place in places}))
        low = min(place[short] for place in places)
        if len({place[short] for place in places}) == 2:
            there = sorted((i for i in range(count) if places[i][short] == low), key=lambda i: places[i][long])
            back = sorted((i for i in range(count) if places[i][short] != low), key=lambda i: -places[i][long])
            return there + back
    return list(range(count))


def make_on_device(order, node_size):
    count = len(order)
    half_way = count // 2
    onward = [(order[i], order[(i + 1) % count]) for i in range(count)]
    backward = [(order[i], order[i - 1]) for i in range(count)]

    def on(x):
        return lax.ppermute(x, "ep", onward)

    def back(x):
        return lax.ppermute(x, "ep", backward)

    def gather(own):
        rows = own.shape[0] // 2
        behind, ahead = own, own
        blocks = [own]
        for _ in range(half_way - 1):
            behind, ahead = on(behind), back(ahead)
            blocks += [behind, ahead]
        blocks += [on(behind[:rows]), back(ahead[rows:])]
        return blocks

    def scatter(sums, tokens):
        rows = tokens // 2

        def block(distance, side):
            first = tokens * (2 * distance - 1 + side)
            return sums[first : first + tokens]

        opposite = sums[tokens * (count - 1) :]
        going_on = on(opposite[:rows].astype(jnp.bfloat16)).astype(jnp.float32)
        going_back = back(opposite[rows:].astype(jnp.bfloat16)).astype(jnp.float32)
        going_on = jnp.pad(going_on, ((0, tokens - rows), (0, 0)))
        going_back = jnp.pad(going_back, ((rows, 0), (0, 0)))
        for distance in range(half_way - 1, 0, -1):
            going_on = on((going_on + block(distance, 1)).astype(jnp.bfloat16)).astype(jnp.float32)
            going_back = back((going_back + block(distance, 0)).astype(jnp.bfloat16)).astype(jnp.float32)
        return (sums[:tokens] + going_on + going_back).astype(jnp.bfloat16)

    def on_device(tokens, expert_ids, gate_weights, gate_up_weight, down_weight):
        token_count, width = tokens.shape
        top = expert_ids.shape[1]
        local_count = gate_up_weight.shape[0]
        inner = down_weight.shape[1]
        me = lax.axis_index("ep")
        core = lax.axis_index("node")
        experts = []
        for shift in range(node_size):
            if shift:
                ring = [(i, (i - shift) % node_size) for i in range(node_size)]
                up, down = lax.ppermute((gate_up_weight, down_weight), "node", ring)
            else:
                up, down = gate_up_weight, down_weight
            holder = me * node_size + lax.rem(core + shift, node_size)
            for local in range(local_count):
                experts.append((holder * local_count + local, up[local], down[local]))
        parts = []
        rest = gate_weights
        for _ in range(3):
            part = lax.reduce_precision(rest, 8, 7)
            rest = rest - part
            parts.append(part)
        side = jnp.concatenate([expert_ids.astype(jnp.float32)] + parts, axis=1).astype(jnp.bfloat16)
        side = jnp.pad(side, ((0, 0), (0, -side.shape[1] % 128)))
        step = width // CHUNKS
        totals = [None] * len(experts)
        for chunk in range(CHUNKS):
            own = tokens[:, chunk * step : (chunk + 1) * step]
            if chunk == 0:
                own = jnp.concatenate([own, side], axis=1)
            rows = jnp.concatenate(gather(own), axis=0)
            if chunk == 0:
                rows, sides = rows[:, :step], rows[:, step:].astype(jnp.float32)
            for i, (_, up, _) in enumerate(experts):
                part = jnp.dot(rows, up[chunk * step : (chunk + 1) * step], preferred_element_type=jnp.float32)
                totals[i] = part if totals[i] is None else totals[i] + part
        weights = sides[:, top : 2 * top] + sides[:, 2 * top : 3 * top] + sides[:, 3 * top : 4 * top]
        hidden, scales = [], []
        for (number, _, _), total in zip(experts, totals):
            hidden.append((jax.nn.silu(total[:, :inner]) * total[:, inner:]).astype(jnp.bfloat16))
            chosen = sides[:, :top] == number.astype(jnp.float32)
            scales.append(jnp.sum(jnp.where(chosen, weights, 0.0), axis=1, keepdims=True))
        outs = []
        for chunk in range(CHUNKS):
            sums = None
            for (_, _, down), rows, scale in zip(experts, hidden, scales):
                part = scale * jnp.dot(
                    rows, down[:, chunk * step : (chunk + 1) * step], preferred_element_type=jnp.float32
                )
                sums = part if sums is None else sums + part
            outs.append(scatter(sums, token_count))
        return jnp.concatenate(outs, axis=1)

    return on_device


def solution(mesh):
    placed = (
        P(("groups", "ep", "node"), None),
        P(("groups", "ep", "node"), None),
        P(("groups", "ep", "node"), None),
        P(("ep", "node"), None, None),
        P(("ep", "node"), None, None),
    )
    return jax.shard_map(
        make_on_device(ring_order(mesh), mesh.shape["node"]),
        mesh=mesh,
        in_specs=placed,
        out_specs=P(("groups", "ep", "node"), None),
        check_vma=False,
    )
```

```python
import functools

import jax
import jax.numpy as jnp
from jax import lax
from jax.experimental import pallas as pl
from jax.experimental.pallas import tpu as pltpu
from jax.sharding import PartitionSpec as P


SUBSETS = 2
LANES = 128
ROWS = 128


def ring_order(mesh):
    at = mesh.axis_names.index("ep")
    count = mesh.devices.shape[at]
    line = [mesh.devices[tuple(i if d == at else 0 for d in range(mesh.devices.ndim))] for i in range(count)]
    places = [getattr(device, "coords", None) for device in line]
    if any(place is None for place in places):
        return list(range(count))
    varying = [d for d in range(3) if len({place[d] for place in places}) > 1]
    if len(varying) == 2:
        short, long = sorted(varying, key=lambda d: len({place[d] for place in places}))
        low = min(place[short] for place in places)
        if len({place[short] for place in places}) == 2:
            there = sorted((i for i in range(count) if places[i][short] == low), key=lambda i: places[i][long])
            back = sorted((i for i in range(count) if places[i][short] != low), key=lambda i: -places[i][long])
            return there + back
    return list(range(count))


def resident(x):
    pieces = 8
    rows = x.shape[0] // pieces

    def body(x_ref, o_ref, sems):
        copies = [
            pltpu.make_async_copy(
                x_ref.at[pl.ds(i * rows, rows)], o_ref.at[pl.ds(i * rows, rows)], sems.at[i]
            )
            for i in range(pieces)
        ]
        for copy in copies:
            copy.start()
        for copy in copies:
            copy.wait()

    return pl.pallas_call(
        body,
        out_shape=pltpu.VMEM(x.shape, x.dtype),
        in_specs=[pl.BlockSpec(memory_space=pltpu.HBM)],
        out_specs=pl.BlockSpec(memory_space=pltpu.VMEM),
        scratch_shapes=[pltpu.SemaphoreType.DMA((pieces,))],
        compiler_params=pltpu.CompilerParams(vmem_limit_bytes=1 << 20),
        cost_estimate=pl.CostEstimate(flops=500 * x.size, bytes_accessed=4 * x.size, transcendentals=0),
    )(pltpu.with_memory_space_constraint(x, pltpu.HBM))


def expert_body(width, inner, node_size, local_count, block_count, *refs):
    expert_count = node_size * local_count
    expert_total = lax.axis_size("ep") * expert_count
    blocks = refs[:block_count]
    ups = refs[block_count : block_count + expert_count]
    downs = refs[block_count + expert_count : block_count + 2 * expert_count]
    out_refs, x_ref = refs[block_count + 2 * expert_count : -1], refs[-1]
    me = lax.axis_index("ep") * node_size
    core = lax.axis_index("node")
    numbers = [
        (me + lax.rem(core + shift, node_size)) * local_count + local
        for shift in range(node_size)
        for local in range(local_count)
    ]
    row = 0
    for block in blocks:
        x_ref[row : row + block.shape[0], :] = block[...]
        row += block.shape[0]
    side = x_ref[:, width:].astype(jnp.float32)
    lane = lax.broadcasted_iota(jnp.int32, side.shape, 1)
    hidden, scales = [], []
    for e in range(expert_count):
        total = jnp.dot(x_ref[:, :width], ups[e][...], preferred_element_type=jnp.float32)
        hidden.append((jax.nn.silu(total[:, :inner]) * total[:, inner:]).astype(jnp.bfloat16))
        mine = (lane == numbers[e]) | (lane == numbers[e] + expert_total) | (lane == numbers[e] + 2 * expert_total)
        scales.append(jnp.sum(jnp.where(mine, side, 0.0), axis=1, keepdims=True))
    tile = 512 if width % 512 == 0 else LANES
    for n in range(width // tile):
        at = slice(n * tile, (n + 1) * tile)
        y = None
        for e in range(expert_count):
            part = scales[e] * jnp.dot(hidden[e], downs[e][:, at], preferred_element_type=jnp.float32)
            y = part if y is None else y + part
        row = 0
        for out in out_refs:
            out[:, at] = y[row : row + out.shape[0]].astype(out.dtype)
            row += out.shape[0]


def apply_experts(blocks, dtypes, ups, downs, node_size):
    inner, width = downs[0].shape
    rows = sum(block.shape[0] for block in blocks)
    vmem = pl.BlockSpec(memory_space=pltpu.VMEM)
    weights = [pltpu.with_memory_space_constraint(x, pltpu.VMEM) for x in (*ups, *downs)]
    inputs = [*blocks, *weights]
    return pl.pallas_call(
        functools.partial(expert_body, width, inner, node_size, len(ups) // node_size, len(blocks)),
        out_shape=[jax.ShapeDtypeStruct((b.shape[0], width), dtype) for b, dtype in zip(blocks, dtypes)],
        in_specs=[vmem] * len(inputs),
        out_specs=[vmem] * len(blocks),
        scratch_shapes=[pltpu.VMEM((rows, blocks[0].shape[1]), jnp.bfloat16)],
        compiler_params=pltpu.CompilerParams(vmem_limit_bytes=12 << 20),
        cost_estimate=pl.CostEstimate(
            flops=6 * rows * width * inner * len(ups), bytes_accessed=rows * width * 6, transcendentals=rows * inner
        ),
    )(*inputs)


def make_on_device(order, node_size):
    count = len(order)
    half_way = count // 2
    onward = [(order[i], order[(i + 1) % count]) for i in range(count)]
    backward = [(order[i], order[i - 1]) for i in range(count)]

    def on(x):
        return lax.ppermute(x, "ep", onward)

    def back(x):
        return lax.ppermute(x, "ep", backward)

    def gather(own):
        rows = own.shape[0] // 2
        left, right = own, own
        blocks = [own]
        for i in range(half_way):
            if i == half_way - 1:
                left, right = left[:rows], right[rows:]
            left = on(left)
            right = back(right)
            blocks += [left, right]
        return blocks

    def scatter(sums):
        left, right = sums[-2:]
        rows, other = left.shape[0], right.shape[0]
        for i in range(half_way):
            left = on(left)
            right = back(right)
            left, right = left.astype(jnp.float32), right.astype(jnp.float32)
            if i == 0:
                left = jnp.pad(left, ((0, other), (0, 0)))
                right = jnp.pad(right, ((rows, 0), (0, 0)))
            distance = half_way - 1 - i
            if distance:
                left = (left + sums[2 * distance]).astype(jnp.bfloat16)
                right = (right + sums[2 * distance - 1]).astype(jnp.bfloat16)
        return (sums[0] + left + right).astype(jnp.bfloat16)

    def on_device(tokens, expert_ids, gate_weights, gate_up_weight, down_weight):
        token_count, _ = tokens.shape
        local_count = gate_up_weight.shape[0]
        expert_total = count * node_size * local_count
        chosen = expert_ids[:, :, None] == jnp.arange(expert_total, dtype=jnp.int32)
        rest = jnp.sum(jnp.where(chosen, gate_weights[:, :, None], 0.0), axis=1)
        parts = []
        for _ in range(3):
            part = lax.reduce_precision(rest, 8, 7)
            rest = rest - part
            parts.append(part)
        side = jnp.concatenate(parts, axis=1).astype(jnp.bfloat16)
        side = jnp.pad(side, ((0, 0), (0, -side.shape[1] % LANES)))
        ups, downs = [], []
        for shift in range(node_size):
            up, down = gate_up_weight, down_weight
            if shift:
                ring = [(i, (i - shift) % node_size) for i in range(node_size)]
                up, down = lax.ppermute((up, down), "node", ring)
            for local in range(local_count):
                for held, weight in ((ups, up[local]), (downs, down[local])):
                    held.append(resident(weight))
        rows = token_count // SUBSETS
        gathered = []
        for s in range(SUBSETS):
            at = slice(s * rows, (s + 1) * rows)
            gathered.append(gather(jnp.concatenate([tokens[at], side[at]], axis=1)))
        outs = []
        for s in range(SUBSETS):
            blocks, sums = gathered[s], []
            dtypes = [jnp.float32] * (len(blocks) - 2) + [jnp.bfloat16] * 2
            per_call = max(1, ROWS // rows) + 1
            starts = list(range(len(blocks), 0, -per_call))
            for end in reversed(starts):
                at = slice(max(0, end - per_call), end)
                sums += apply_experts(blocks[at], dtypes[at], ups, downs, node_size)
            outs.append(scatter(sums))
        return jnp.concatenate(outs, axis=0)

    return on_device


def solution(mesh):
    placed = (
        P(("groups", "ep", "node"), None),
        P(("groups", "ep", "node"), None),
        P(("groups", "ep", "node"), None),
        P(("ep", "node"), None, None),
        P(("ep", "node"), None, None),
    )
    return jax.shard_map(
        make_on_device(ring_order(mesh), mesh.shape["node"]),
        mesh=mesh,
        in_specs=placed,
        out_specs=P(("groups", "ep", "node"), None),
        check_vma=False,
    )
```

```python
import functools

import jax
import jax.numpy as jnp
from jax import lax
from jax.experimental import pallas as pl
from jax.experimental.pallas import tpu as pltpu
from jax.sharding import PartitionSpec as P


SUBSETS = 2
LANES = 128
ROWS = 128


def ring_order(mesh):
    at = mesh.axis_names.index("ep")
    count = mesh.devices.shape[at]
    line = [mesh.devices[tuple(i if d == at else 0 for d in range(mesh.devices.ndim))] for i in range(count)]
    places = [getattr(device, "coords", None) for device in line]
    if any(place is None for place in places):
        return list(range(count))
    varying = [d for d in range(3) if len({place[d] for place in places}) > 1]
    if len(varying) == 2:
        short, long = sorted(varying, key=lambda d: len({place[d] for place in places}))
        low = min(place[short] for place in places)
        if len({place[short] for place in places}) == 2:
            there = sorted((i for i in range(count) if places[i][short] == low), key=lambda i: places[i][long])
            back = sorted((i for i in range(count) if places[i][short] != low), key=lambda i: -places[i][long])
            return there + back
    return list(range(count))


def resident(x):
    pieces = 8
    rows = x.shape[0] // pieces

    def body(x_ref, o_ref, sems):
        copies = [
            pltpu.make_async_copy(
                x_ref.at[pl.ds(i * rows, rows)], o_ref.at[pl.ds(i * rows, rows)], sems.at[i]
            )
            for i in range(pieces)
        ]
        for copy in copies:
            copy.start()
        for copy in copies:
            copy.wait()

    return pl.pallas_call(
        body,
        out_shape=pltpu.VMEM(x.shape, x.dtype),
        in_specs=[pl.BlockSpec(memory_space=pltpu.HBM)],
        out_specs=pl.BlockSpec(memory_space=pltpu.VMEM),
        scratch_shapes=[pltpu.SemaphoreType.DMA((pieces,))],
        compiler_params=pltpu.CompilerParams(vmem_limit_bytes=1 << 20),
        cost_estimate=pl.CostEstimate(flops=500 * x.size, bytes_accessed=4 * x.size, transcendentals=0),
    )(pltpu.with_memory_space_constraint(x, pltpu.HBM))


def pack_body(expert_total, ids_ref, gates_ref, tokens_ref, *refs):
    out_refs, (ids_held, gates_held, sems) = refs[:SUBSETS], refs[SUBSETS:]
    rows = out_refs[0].shape[0]
    width = tokens_ref.shape[1]
    first = [
        pltpu.make_async_copy(ids_ref, ids_held, sems.at[SUBSETS]),
        pltpu.make_async_copy(gates_ref, gates_held, sems.at[SUBSETS + 1]),
    ]
    then = [
        pltpu.make_async_copy(tokens_ref.at[pl.ds(s * rows, rows)], out.at[:, pl.ds(0, width)], sems.at[s])
        for s, out in enumerate(out_refs)
    ]
    for copy in first + then:
        copy.start()
    for copy in first:
        copy.wait()
    ids, gates = ids_held[...], gates_held[...]
    rest = jnp.concatenate(
        [jnp.sum(jnp.where(ids == e, gates, 0.0), axis=0, keepdims=True) for e in range(expert_total)], axis=0
    )
    parts = []
    for _ in range(3):
        part = rest.astype(jnp.bfloat16).astype(jnp.float32)
        rest = rest - part
        parts.append(part)
    side = jnp.concatenate(parts, axis=0).T
    side = jnp.concatenate([side[s * rows : (s + 1) * rows] for s in range(SUBSETS)], axis=1)
    empty = out_refs[0].shape[1] - width - side.shape[1]
    if empty:
        side = jnp.concatenate([side, jnp.zeros((rows, empty), jnp.float32)], axis=1)
    out_refs[0][:, width:] = side.astype(jnp.bfloat16)
    for copy in then:
        copy.wait()


def pack(tokens, expert_ids, gate_weights, expert_total):
    token_count, width = tokens.shape
    rows = token_count // SUBSETS
    inputs = [pltpu.with_memory_space_constraint(x, pltpu.HBM) for x in (expert_ids.T, gate_weights.T, tokens)]
    return pl.pallas_call(
        functools.partial(pack_body, expert_total),
        out_shape=[
            jax.ShapeDtypeStruct((rows, width + (0 if s else side_columns(expert_total))), tokens.dtype)
            for s in range(SUBSETS)
        ],
        in_specs=[pl.BlockSpec(memory_space=pltpu.HBM)] * 3,
        out_specs=[pl.BlockSpec(memory_space=pltpu.VMEM)] * SUBSETS,
        scratch_shapes=[
            pltpu.VMEM(inputs[0].shape, jnp.int32),
            pltpu.VMEM(inputs[1].shape, jnp.float32),
            pltpu.SemaphoreType.DMA((SUBSETS + 2,)),
        ],
        compiler_params=pltpu.CompilerParams(vmem_limit_bytes=4 << 20),
    )(*inputs)


def expert_body(subset, node_size, local_count, block_count, side_count, *refs):
    expert_count = node_size * local_count
    expert_total = lax.axis_size("ep") * expert_count
    blocks = refs[:block_count]
    sides = refs[block_count : block_count + side_count]
    weights = refs[block_count + side_count :]
    ups = weights[:expert_count]
    downs = weights[expert_count : 2 * expert_count]
    out_refs = weights[2 * expert_count :]
    inner, width = downs[0].shape
    me = lax.axis_index("ep") * node_size
    core = lax.axis_index("node")
    numbers = [
        (me + lax.rem(core + shift, node_size)) * local_count + local
        for shift in range(node_size)
        for local in range(local_count)
    ]
    side_width = side_columns(expert_total)
    side = jnp.concatenate([ref[:, ref.shape[1] - side_width :] for ref in sides], axis=0).astype(jnp.float32)
    lane = lax.broadcasted_iota(jnp.int32, side.shape, 1) - subset * 3 * expert_total
    depth = 1024 if width % 1024 == 0 else width
    totals = [None] * expert_count
    for k in range(width // depth):
        at = slice(k * depth, (k + 1) * depth)
        x = jnp.concatenate([block[:, at] for block in blocks], axis=0)
        for e in range(expert_count):
            part = jnp.dot(x, ups[e][at, :], preferred_element_type=jnp.float32)
            totals[e] = part if totals[e] is None else totals[e] + part
    hidden = []
    for e, total in enumerate(totals):
        mine = (lane == numbers[e]) | (lane == numbers[e] + expert_total) | (lane == numbers[e] + 2 * expert_total)
        scale = jnp.sum(jnp.where(mine, side, 0.0), axis=1, keepdims=True)
        hidden.append((scale * (jax.nn.silu(total[:, :inner]) * total[:, inner:])).astype(jnp.bfloat16))
    tile = 512 if width % 512 == 0 else LANES
    for n in range(width // tile):
        at = slice(n * tile, (n + 1) * tile)
        y = None
        for e in range(expert_count):
            part = jnp.dot(hidden[e], downs[e][:, at], preferred_element_type=jnp.float32)
            y = part if y is None else y + part
        row = 0
        for out in out_refs:
            out[:, at] = y[row : row + out.shape[0]].astype(out.dtype)
            row += out.shape[0]


def side_columns(expert_total):
    return -(-SUBSETS * 3 * expert_total // LANES) * LANES


def apply_experts(subset, blocks, sides, dtypes, ups, downs, node_size):
    inner, width = downs[0].shape
    rows = sum(block.shape[0] for block in blocks)
    vmem = pl.BlockSpec(memory_space=pltpu.VMEM)
    weights = [pltpu.with_memory_space_constraint(x, pltpu.VMEM) for x in (*ups, *downs)]
    inputs = [*blocks, *sides, *weights]
    return pl.pallas_call(
        functools.partial(expert_body, subset, node_size, len(ups) // node_size, len(blocks), len(sides)),
        out_shape=[jax.ShapeDtypeStruct((b.shape[0], width), dtype) for b, dtype in zip(blocks, dtypes)],
        in_specs=[vmem] * len(inputs),
        out_specs=[vmem] * len(blocks),
        compiler_params=pltpu.CompilerParams(vmem_limit_bytes=12 << 20),
        cost_estimate=pl.CostEstimate(
            flops=6 * rows * width * inner * len(ups), bytes_accessed=rows * width * 6, transcendentals=rows * inner
        ),
    )(*inputs)


def make_on_device(order, node_size):
    count = len(order)
    half_way = count // 2
    onward = [(order[i], order[(i + 1) % count]) for i in range(count)]
    backward = [(order[i], order[i - 1]) for i in range(count)]

    def on(x):
        return lax.ppermute(x, "ep", onward)

    def back(x):
        return lax.ppermute(x, "ep", backward)

    def gather(own):
        rows = own.shape[0] // 2
        left, right = own, own
        blocks = [own]
        for i in range(half_way):
            if i == half_way - 1:
                left, right = left[:rows], right[rows:]
            left = on(left)
            right = back(right)
            blocks += [left, right]
        return blocks

    def scatter(sums):
        left, right = sums[-2:]
        rows, other = left.shape[0], right.shape[0]
        for i in range(half_way):
            left = on(left)
            right = back(right)
            left, right = left.astype(jnp.float32), right.astype(jnp.float32)
            if i == 0:
                left = jnp.pad(left, ((0, other), (0, 0)))
                right = jnp.pad(right, ((rows, 0), (0, 0)))
            distance = half_way - 1 - i
            if distance:
                left = (left + sums[2 * distance]).astype(jnp.bfloat16)
                right = (right + sums[2 * distance - 1]).astype(jnp.bfloat16)
        return (sums[0] + left + right).astype(jnp.bfloat16)

    def on_device(tokens, expert_ids, gate_weights, gate_up_weight, down_weight):
        token_count, _ = tokens.shape
        local_count = gate_up_weight.shape[0]
        expert_total = count * node_size * local_count
        rows = token_count // SUBSETS
        subsets = pack(tokens, expert_ids, gate_weights, expert_total)
        gathered = [gather(own) for own in subsets]
        sides = gathered[0]
        ups, downs = [], []
        for shift in range(node_size):
            up, down = gate_up_weight, down_weight
            if shift:
                ring = [(i, (i - shift) % node_size) for i in range(node_size)]
                up = lax.ppermute(up, "node", ring)
                down = lax.ppermute(down, "node", ring)
            for local in range(local_count):
                for held, weight in ((ups, up[local]), (downs, down[local])):
                    if not shift:
                        weight = resident(weight)
                    held.append(weight)
        outs = []
        for s in range(SUBSETS):
            blocks, sums = gathered[s], []
            dtypes = [jnp.float32] * (len(blocks) - 2) + [jnp.bfloat16] * 2
            per_call = max(1, ROWS // rows) + 1
            starts = list(range(len(blocks), 0, -per_call))
            for end in reversed(starts):
                at = slice(max(0, end - per_call), end)
                sums += apply_experts(s, blocks[at], sides[at], dtypes[at], ups, downs, node_size)
            outs.append(scatter(sums))
        return jnp.concatenate(outs, axis=0)

    return on_device


def solution(mesh):
    placed = (
        P(("groups", "ep", "node"), None),
        P(("groups", "ep", "node"), None),
        P(("groups", "ep", "node"), None),
        P(("ep", "node"), None, None),
        P(("ep", "node"), None, None),
    )
    return jax.shard_map(
        make_on_device(ring_order(mesh), mesh.shape["node"]),
        mesh=mesh,
        in_specs=placed,
        out_specs=P(("groups", "ep", "node"), None),
        check_vma=False,
    )
```

```python
import functools

import jax
import jax.numpy as jnp
from jax import lax
from jax.experimental import pallas as pl
from jax.experimental.pallas import tpu as pltpu
from jax.sharding import PartitionSpec as P


SUBSETS = 2
LANES = 128
ROWS = 128
DEPTH = 512
TILE = 512


def ring_order(mesh):
    at = mesh.axis_names.index("ep")
    count = mesh.devices.shape[at]
    line = [mesh.devices[tuple(i if d == at else 0 for d in range(mesh.devices.ndim))] for i in range(count)]
    places = [getattr(device, "coords", None) for device in line]
    if any(place is None for place in places):
        return list(range(count))
    varying = [d for d in range(3) if len({place[d] for place in places}) > 1]
    if len(varying) == 2:
        short, long = sorted(varying, key=lambda d: len({place[d] for place in places}))
        low = min(place[short] for place in places)
        if len({place[short] for place in places}) == 2:
            there = sorted((i for i in range(count) if places[i][short] == low), key=lambda i: places[i][long])
            back = sorted((i for i in range(count) if places[i][short] != low), key=lambda i: -places[i][long])
            return there + back
    return list(range(count))


def resident(x):
    pieces = 8
    rows = x.shape[0] // pieces

    def body(x_ref, o_ref, sems):
        copies = [
            pltpu.make_async_copy(
                x_ref.at[pl.ds(i * rows, rows)], o_ref.at[pl.ds(i * rows, rows)], sems.at[i]
            )
            for i in range(pieces)
        ]
        for copy in copies:
            copy.start()
        for copy in copies:
            copy.wait()

    return pl.pallas_call(
        body,
        out_shape=pltpu.VMEM(x.shape, x.dtype),
        in_specs=[pl.BlockSpec(memory_space=pltpu.HBM)],
        out_specs=pl.BlockSpec(memory_space=pltpu.VMEM),
        scratch_shapes=[pltpu.SemaphoreType.DMA((pieces,))],
        compiler_params=pltpu.CompilerParams(vmem_limit_bytes=1 << 20),
        cost_estimate=pl.CostEstimate(flops=500 * x.size, bytes_accessed=4 * x.size, transcendentals=0),
    )(pltpu.with_memory_space_constraint(x, pltpu.HBM))


def pack_body(expert_total, ids_ref, gates_ref, tokens_ref, *refs):
    out_refs, (ids_held, gates_held, sems) = refs[:SUBSETS], refs[SUBSETS:]
    rows = out_refs[0].shape[0]
    width = tokens_ref.shape[1]
    first = [
        pltpu.make_async_copy(ids_ref, ids_held, sems.at[SUBSETS]),
        pltpu.make_async_copy(gates_ref, gates_held, sems.at[SUBSETS + 1]),
    ]
    then = [
        pltpu.make_async_copy(tokens_ref.at[pl.ds(s * rows, rows)], out.at[:, pl.ds(0, width)], sems.at[s])
        for s, out in enumerate(out_refs)
    ]
    for copy in first + then:
        copy.start()
    for copy in first:
        copy.wait()
    ids, gates = ids_held[...], gates_held[...]
    rest = jnp.concatenate(
        [jnp.sum(jnp.where(ids == e, gates, 0.0), axis=0, keepdims=True) for e in range(expert_total)], axis=0
    )
    parts = []
    for _ in range(3):
        part = rest.astype(jnp.bfloat16).astype(jnp.float32)
        rest = rest - part
        parts.append(part)
    side = jnp.concatenate(parts, axis=0).T
    side = jnp.concatenate([side[s * rows : (s + 1) * rows] for s in range(SUBSETS)], axis=1)
    empty = out_refs[0].shape[1] - width - side.shape[1]
    if empty:
        side = jnp.concatenate([side, jnp.zeros((rows, empty), jnp.float32)], axis=1)
    out_refs[0][:, width:] = side.astype(jnp.bfloat16)
    for copy in then:
        copy.wait()


def pack(tokens, expert_ids, gate_weights, expert_total):
    token_count, width = tokens.shape
    rows = token_count // SUBSETS
    inputs = [pltpu.with_memory_space_constraint(x, pltpu.HBM) for x in (expert_ids.T, gate_weights.T, tokens)]
    return pl.pallas_call(
        functools.partial(pack_body, expert_total),
        out_shape=[
            jax.ShapeDtypeStruct((rows, width + (0 if s else side_columns(expert_total))), tokens.dtype)
            for s in range(SUBSETS)
        ],
        in_specs=[pl.BlockSpec(memory_space=pltpu.HBM)] * 3,
        out_specs=[pl.BlockSpec(memory_space=pltpu.VMEM)] * SUBSETS,
        scratch_shapes=[
            pltpu.VMEM(inputs[0].shape, jnp.int32),
            pltpu.VMEM(inputs[1].shape, jnp.float32),
            pltpu.SemaphoreType.DMA((SUBSETS + 2,)),
        ],
        compiler_params=pltpu.CompilerParams(vmem_limit_bytes=4 << 20),
    )(*inputs)


def expert_body(subset, node_size, local_count, block_count, late, side_count, *refs):
    expert_count = node_size * local_count
    expert_total = lax.axis_size("ep") * expert_count
    blocks = refs[:block_count]
    sides = refs[block_count : block_count + side_count]
    weights = refs[block_count + side_count :]
    ups = weights[:expert_count]
    downs = weights[expert_count : 2 * expert_count]
    out_refs = weights[2 * expert_count :]
    inner, width = downs[0].shape
    me = lax.axis_index("ep") * node_size
    core = lax.axis_index("node")
    numbers = [
        (me + lax.rem(core + shift, node_size)) * local_count + local
        for shift in range(node_size)
        for local in range(local_count)
    ]
    side_width = side_columns(expert_total)
    side = jnp.concatenate([ref[:, ref.shape[1] - side_width :] for ref in sides], axis=0).astype(jnp.float32)
    lane = lax.broadcasted_iota(jnp.int32, side.shape, 1) - subset * 3 * expert_total
    totals = [None] * expert_count
    for k in range(0, width, DEPTH):
        at = slice(k, k + DEPTH)
        parts = [block[:, at] for block in blocks[: block_count - late]]
        if late:
            parts.append(blocks[-1][:, at])
        x = jnp.concatenate(parts, axis=0)
        for e in range(expert_count):
            part = jnp.dot(x, ups[e][at, :], preferred_element_type=jnp.float32)
            totals[e] = part if totals[e] is None else totals[e] + part
    hidden = []
    for e, total in enumerate(totals):
        mine = (lane == numbers[e]) | (lane == numbers[e] + expert_total) | (lane == numbers[e] + 2 * expert_total)
        scale = jnp.sum(jnp.where(mine, side, 0.0), axis=1, keepdims=True)
        rounded = (jax.nn.silu(total[:, :inner]) * total[:, inner:]).astype(jnp.bfloat16)
        hidden.append((scale * rounded.astype(jnp.float32)).astype(jnp.bfloat16))
    for n in range(0, width, TILE):
        at = slice(n, n + TILE)
        y = None
        for e in range(expert_count):
            part = jnp.dot(hidden[e], downs[e][:, at], preferred_element_type=jnp.float32)
            y = part if y is None else y + part
        row = 0
        for out in out_refs[: block_count - late]:
            out[:, at] = y[row : row + out.shape[0]]
            row += out.shape[0]
        if late:
            out_refs[-1][:, at] = y[row:].astype(jnp.bfloat16)


def side_columns(expert_total):
    return -(-SUBSETS * 3 * expert_total // LANES) * LANES


def apply_experts(subset, blocks, late, sides, ups, downs, node_size):
    inner, width = downs[0].shape
    rows = sum(block.shape[0] for block in (*blocks, *late))
    out_shape = [jax.ShapeDtypeStruct((block.shape[0], width), jnp.float32) for block in blocks]
    if late:
        out_shape += [jax.ShapeDtypeStruct((late[0].shape[0], width), jnp.bfloat16)]
    vmem = pl.BlockSpec(memory_space=pltpu.VMEM)
    weights = [pltpu.with_memory_space_constraint(x, pltpu.VMEM) for x in (*ups, *downs)]
    inputs = [*blocks, *late, *sides, *weights]
    return pl.pallas_call(
        functools.partial(
            expert_body, subset, node_size, len(ups) // node_size, len(blocks) + len(late), bool(late), len(sides)
        ),
        out_shape=out_shape,
        in_specs=[vmem] * len(inputs),
        out_specs=[vmem] * len(out_shape),
        compiler_params=pltpu.CompilerParams(vmem_limit_bytes=12 << 20),
        cost_estimate=pl.CostEstimate(
            flops=6 * rows * width * inner * len(ups), bytes_accessed=rows * width * 6, transcendentals=rows * inner
        ),
    )(*inputs)


def make_on_device(order, node_size):
    count = len(order)
    half_way = count // 2
    onward = [(order[i], order[(i + 1) % count]) for i in range(count)]
    backward = [(order[i], order[i - 1]) for i in range(count)]

    def on(x):
        return lax.ppermute(x, "ep", onward)

    def back(x):
        return lax.ppermute(x, "ep", backward)

    def gather(own, onward_last):
        left, right = own, own
        blocks = [own]
        for i in range(half_way):
            last = i == half_way - 1
            if not last or onward_last:
                left = on(left)
            if not last or not onward_last:
                right = back(right)
            blocks += [left if onward_last else right] if last else [left, right]
        return blocks

    def scatter(sums, onward_first):
        left, right = (sums[-1], None) if onward_first else (None, sums[-1])
        for i in range(half_way):
            distance = half_way - i
            if i:
                left = (sums[2 * distance] if left is None else left + sums[2 * distance]).astype(jnp.bfloat16)
                right = (sums[2 * distance - 1] if right is None else right + sums[2 * distance - 1]).astype(jnp.bfloat16)
            if left is not None:
                left = on(left).astype(jnp.float32)
            if right is not None:
                right = back(right).astype(jnp.float32)
        return (sums[0] + left + right).astype(jnp.bfloat16)

    def on_device(tokens, expert_ids, gate_weights, gate_up_weight, down_weight):
        token_count, _ = tokens.shape
        local_count = gate_up_weight.shape[0]
        expert_total = count * node_size * local_count
        rows = token_count // SUBSETS
        subsets = pack(tokens, expert_ids, gate_weights, expert_total)
        gathered = [gather(own, s == 0) for s, own in enumerate(subsets)]
        sides = gathered[0]
        ups, downs = [], []
        for shift in range(node_size):
            up, down = gate_up_weight, down_weight
            if shift:
                ring = [(i, (i - shift) % node_size) for i in range(node_size)]
                up = lax.ppermute(up, "node", ring)
                down = lax.ppermute(down, "node", ring)
            for local in range(local_count):
                for held, weight in ((ups, up[local]), (downs, down[local])):
                    if not shift:
                        weight = resident(weight)
                    held.append(weight)
        outs = []
        for s in range(SUBSETS):
            blocks, late, sums = gathered[s][:-1], gathered[s][-1:], []
            per_call = max(1, ROWS // rows)
            total = len(blocks) + 1
            for first in range(0, total, per_call):
                end = min(first + per_call, total)
                sums += apply_experts(
                    s, blocks[first:end], late if end == total else [], sides[first:end], ups, downs, node_size
                )
            outs.append(scatter(sums, s == 0))
        result = jnp.zeros(tokens.shape, tokens.dtype)
        for s, out in enumerate(outs):
            result = lax.optimization_barrier(lax.dynamic_update_slice(result, out, (s * rows, 0)))
        return result

    return on_device


def solution(mesh):
    placed = (
        P(("groups", "ep", "node"), None),
        P(("groups", "ep", "node"), None),
        P(("groups", "ep", "node"), None),
        P(("ep", "node"), None, None),
        P(("ep", "node"), None, None),
    )
    return jax.shard_map(
        make_on_device(ring_order(mesh), mesh.shape["node"]),
        mesh=mesh,
        in_specs=placed,
        out_specs=P(("groups", "ep", "node"), None),
        check_vma=False,
    )
```

```python
import functools

import jax
import jax.numpy as jnp
from jax import lax
from jax.experimental import pallas as pl
from jax.experimental.pallas import tpu as pltpu
from jax.sharding import PartitionSpec as P


SUBSETS = 2
LANES = 128
ROWS = 128
GATHER_SHARES = (0.72, 0.58)
SCATTER_SHARES = (0.65, 0.5)
DEPTH = 512
TILE = 512


def ring_order(mesh):
    at = mesh.axis_names.index("ep")
    count = mesh.devices.shape[at]
    line = [mesh.devices[tuple(i if d == at else 0 for d in range(mesh.devices.ndim))] for i in range(count)]
    places = [getattr(device, "coords", None) for device in line]
    if any(place is None for place in places):
        return list(range(count))
    varying = [d for d in range(3) if len({place[d] for place in places}) > 1]
    if len(varying) == 2:
        short, long = sorted(varying, key=lambda d: len({place[d] for place in places}))
        low = min(place[short] for place in places)
        if len({place[short] for place in places}) == 2:
            there = sorted((i for i in range(count) if places[i][short] == low), key=lambda i: places[i][long])
            back = sorted((i for i in range(count) if places[i][short] != low), key=lambda i: -places[i][long])
            return there + back
    return list(range(count))


def resident(x):
    pieces = 8
    rows = x.shape[0] // pieces

    def body(x_ref, o_ref, sems):
        copies = [
            pltpu.make_async_copy(
                x_ref.at[pl.ds(i * rows, rows)], o_ref.at[pl.ds(i * rows, rows)], sems.at[i]
            )
            for i in range(pieces)
        ]
        for copy in copies:
            copy.start()
        for copy in copies:
            copy.wait()

    return pl.pallas_call(
        body,
        out_shape=pltpu.VMEM(x.shape, x.dtype),
        in_specs=[pl.BlockSpec(memory_space=pltpu.HBM)],
        out_specs=pl.BlockSpec(memory_space=pltpu.VMEM),
        scratch_shapes=[pltpu.SemaphoreType.DMA((pieces,))],
        compiler_params=pltpu.CompilerParams(vmem_limit_bytes=1 << 20),
        cost_estimate=pl.CostEstimate(flops=500 * x.size, bytes_accessed=4 * x.size, transcendentals=0),
    )(pltpu.with_memory_space_constraint(x, pltpu.HBM))


def pack_body(expert_total, ids_ref, gates_ref, tokens_ref, *refs):
    out_refs, (ids_held, gates_held, sems) = refs[:SUBSETS], refs[SUBSETS:]
    rows = out_refs[0].shape[0]
    width = tokens_ref.shape[1]
    first = [
        pltpu.make_async_copy(ids_ref, ids_held, sems.at[SUBSETS]),
        pltpu.make_async_copy(gates_ref, gates_held, sems.at[SUBSETS + 1]),
    ]
    then = [
        pltpu.make_async_copy(tokens_ref.at[pl.ds(s * rows, rows)], out.at[:, pl.ds(0, width)], sems.at[s])
        for s, out in enumerate(out_refs)
    ]
    for copy in first + then:
        copy.start()
    for copy in first:
        copy.wait()
    ids, gates = ids_held[...], gates_held[...]
    rest = jnp.concatenate(
        [jnp.sum(jnp.where(ids == e, gates, 0.0), axis=0, keepdims=True) for e in range(expert_total)], axis=0
    )
    parts = []
    for _ in range(3):
        part = rest.astype(jnp.bfloat16).astype(jnp.float32)
        rest = rest - part
        parts.append(part)
    side = jnp.concatenate(parts, axis=0).T
    side = jnp.concatenate([side[s * rows : (s + 1) * rows] for s in range(SUBSETS)], axis=1)
    empty = out_refs[0].shape[1] - width - side.shape[1]
    if empty:
        side = jnp.concatenate([side, jnp.zeros((rows, empty), jnp.float32)], axis=1)
    out_refs[0][:, width:] = side.astype(jnp.bfloat16)
    for copy in then:
        copy.wait()


def pack(tokens, expert_ids, gate_weights, expert_total):
    token_count, width = tokens.shape
    rows = token_count // SUBSETS
    inputs = [pltpu.with_memory_space_constraint(x, pltpu.HBM) for x in (expert_ids.T, gate_weights.T, tokens)]
    return pl.pallas_call(
        functools.partial(pack_body, expert_total),
        out_shape=[
            jax.ShapeDtypeStruct((rows, width + (0 if s else side_columns(expert_total))), tokens.dtype)
            for s in range(SUBSETS)
        ],
        in_specs=[pl.BlockSpec(memory_space=pltpu.HBM)] * 3,
        out_specs=[pl.BlockSpec(memory_space=pltpu.VMEM)] * SUBSETS,
        scratch_shapes=[
            pltpu.VMEM(inputs[0].shape, jnp.int32),
            pltpu.VMEM(inputs[1].shape, jnp.float32),
            pltpu.SemaphoreType.DMA((SUBSETS + 2,)),
        ],
        compiler_params=pltpu.CompilerParams(vmem_limit_bytes=4 << 20),
    )(*inputs)


def share_of(width, share, step):
    return int(width * share) // step * step


def expert_body(subset, node_size, local_count, block_count, late, side_count, *refs):
    expert_count = node_size * local_count
    expert_total = lax.axis_size("ep") * expert_count
    blocks = refs[:block_count]
    sides = refs[block_count : block_count + side_count]
    weights = refs[block_count + side_count :]
    ups = weights[:expert_count]
    downs = weights[expert_count : 2 * expert_count]
    out_refs = weights[2 * expert_count :]
    inner, width = downs[0].shape
    me = lax.axis_index("ep") * node_size
    core = lax.axis_index("node")
    numbers = [
        (me + lax.rem(core + shift, node_size)) * local_count + local
        for shift in range(node_size)
        for local in range(local_count)
    ]
    side_width = side_columns(expert_total)
    side = jnp.concatenate([ref[:, ref.shape[1] - side_width :] for ref in sides], axis=0).astype(jnp.float32)
    lane = lax.broadcasted_iota(jnp.int32, side.shape, 1) - subset * 3 * expert_total
    totals = [None] * expert_count
    for k in range(0, width, DEPTH):
        at = slice(k, k + DEPTH)
        parts = [block[:, at] for block in blocks[: block_count - 2 * late]]
        if late:
            first, then = blocks[-2:]
            cut = first.shape[1]
            parts.append(first[:, at] if k < cut else then[:, k - cut : k - cut + DEPTH])
        x = jnp.concatenate(parts, axis=0)
        for e in range(expert_count):
            part = jnp.dot(x, ups[e][at, :], preferred_element_type=jnp.float32)
            totals[e] = part if totals[e] is None else totals[e] + part
    hidden = []
    for e, total in enumerate(totals):
        mine = (lane == numbers[e]) | (lane == numbers[e] + expert_total) | (lane == numbers[e] + 2 * expert_total)
        scale = jnp.sum(jnp.where(mine, side, 0.0), axis=1, keepdims=True)
        rounded = (jax.nn.silu(total[:, :inner]) * total[:, inner:]).astype(jnp.bfloat16)
        hidden.append((scale * rounded.astype(jnp.float32)).astype(jnp.bfloat16))
    for n in range(0, width, TILE):
        at = slice(n, n + TILE)
        y = None
        for e in range(expert_count):
            part = jnp.dot(hidden[e], downs[e][:, at], preferred_element_type=jnp.float32)
            y = part if y is None else y + part
        row = 0
        for out in out_refs[: block_count - 2 * late]:
            out[:, at] = y[row : row + out.shape[0]]
            row += out.shape[0]
        if late:
            first, then = out_refs[-2:]
            cut = first.shape[1]
            if n < cut:
                first[:, at] = y[row:].astype(first.dtype)
            else:
                then[:, n - cut : n - cut + TILE] = y[row:].astype(then.dtype)


def side_columns(expert_total):
    return -(-SUBSETS * 3 * expert_total // LANES) * LANES


def apply_experts(subset, blocks, late, sides, ups, downs, node_size):
    inner, width = downs[0].shape
    rows = sum(block.shape[0] for block in (*blocks, *late[:1]))
    out_shape = [jax.ShapeDtypeStruct((block.shape[0], width), jnp.float32) for block in blocks]
    if late:
        cut = share_of(width, SCATTER_SHARES[subset], TILE)
        out_shape += [jax.ShapeDtypeStruct((late[0].shape[0], size), jnp.bfloat16) for size in (cut, width - cut)]
    vmem = pl.BlockSpec(memory_space=pltpu.VMEM)
    weights = [pltpu.with_memory_space_constraint(x, pltpu.VMEM) for x in (*ups, *downs)]
    inputs = [*blocks, *late, *sides, *weights]
    return pl.pallas_call(
        functools.partial(
            expert_body, subset, node_size, len(ups) // node_size, len(blocks) + len(late), bool(late), len(sides)
        ),
        out_shape=out_shape,
        in_specs=[vmem] * len(inputs),
        out_specs=[vmem] * len(out_shape),
        compiler_params=pltpu.CompilerParams(vmem_limit_bytes=12 << 20),
        cost_estimate=pl.CostEstimate(
            flops=6 * rows * width * inner * len(ups), bytes_accessed=rows * width * 6, transcendentals=rows * inner
        ),
    )(*inputs)


def make_on_device(order, node_size):
    count = len(order)
    half_way = count // 2
    onward = [(order[i], order[(i + 1) % count]) for i in range(count)]
    backward = [(order[i], order[i - 1]) for i in range(count)]

    def on(x):
        return lax.ppermute(x, "ep", onward)

    def back(x):
        return lax.ppermute(x, "ep", backward)

    def gather(own, cut):
        left, right = own, own
        blocks = [own]
        for i in range(half_way):
            if i == half_way - 1:
                left = left[:, :cut]
                right = right[:, cut:]
            left = on(left)
            right = back(right)
            blocks += [left, right]
        return blocks

    def scatter(sums):
        left, right = sums[-2:]
        cut, other = left.shape[1], right.shape[1]
        for i in range(half_way):
            left = on(left)
            right = back(right)
            left, right = left.astype(jnp.float32), right.astype(jnp.float32)
            if i == 0:
                left = jnp.pad(left, ((0, 0), (0, other)))
                right = jnp.pad(right, ((0, 0), (cut, 0)))
            distance = half_way - 1 - i
            if distance:
                left = (left + sums[2 * distance]).astype(jnp.bfloat16)
                right = (right + sums[2 * distance - 1]).astype(jnp.bfloat16)
        return (sums[0] + left + right).astype(jnp.bfloat16)

    def on_device(tokens, expert_ids, gate_weights, gate_up_weight, down_weight):
        token_count, width = tokens.shape
        local_count = gate_up_weight.shape[0]
        expert_total = count * node_size * local_count
        rows = token_count // SUBSETS
        subsets = pack(tokens, expert_ids, gate_weights, expert_total)
        gathered = [gather(own, share_of(width, GATHER_SHARES[s], DEPTH)) for s, own in enumerate(subsets)]
        sides = gathered[0][:-2] + gathered[0][-1:]
        ups, downs = [], []
        for shift in range(node_size):
            up, down = gate_up_weight, down_weight
            if shift:
                ring = [(i, (i - shift) % node_size) for i in range(node_size)]
                up = lax.ppermute(up, "node", ring)
                down = lax.ppermute(down, "node", ring)
            for local in range(local_count):
                for held, weight in ((ups, up[local]), (downs, down[local])):
                    if not shift:
                        weight = resident(weight)
                    held.append(weight)
        outs = []
        for s in range(SUBSETS):
            blocks, late, sums = gathered[s][:-2], gathered[s][-2:], []
            per_call = max(1, ROWS // rows)
            total = len(blocks) + 1
            for first in range(0, total, per_call):
                end = min(first + per_call, total)
                sums += apply_experts(
                    s, blocks[first:end], late if end == total else [], sides[first:end], ups, downs, node_size
                )
            outs.append(scatter(sums))
        result = jnp.zeros(tokens.shape, tokens.dtype)
        for s, out in enumerate(outs):
            result = lax.optimization_barrier(lax.dynamic_update_slice(result, out, (s * rows, 0)))
        return result

    return on_device


def solution(mesh):
    placed = (
        P(("groups", "ep", "node"), None),
        P(("groups", "ep", "node"), None),
        P(("groups", "ep", "node"), None),
        P(("ep", "node"), None, None),
        P(("ep", "node"), None, None),
    )
    return jax.shard_map(
        make_on_device(ring_order(mesh), mesh.shape["node"]),
        mesh=mesh,
        in_specs=placed,
        out_specs=P(("groups", "ep", "node"), None),
        check_vma=False,
    )
```
